256 devices in a mesh: groups: 4 (over y, x), az: 64 (over z, core).
Axes of the slice: x: 2, y: 2, z: 32, core: 2. Of those that a mesh axis runs over, the one named last changes fastest.
The devices are a block of a 4x8x32 slice.
Arguments:
- sweep_stack: bfloat16 [2, 4, 256, 80, 2560], P(None, None, ('groups', 'az')), parts along dimension 2
- blend_curve: bfloat16 [256, 80], P(('groups', 'az')), parts along dimension 0, may hold values from 0.25 to 4
- sweep_start_index: int32 [256], P(('groups', 'az')), parts along dimension 0, may hold values from -20 to 2530, as said below
- usable_azimuth_extent: int32 [256, 2], P(('groups', 'az')), parts along dimension 0, may hold values from 0 to 80, as said below
- usable_column_extent: int32 [256, 2], P(('groups', 'az')), parts along dimension 0, may hold values from 0 to 2560, as said below
- image_couples: int32 [16, 2], P('groups'), parts along dimension 0, may hold values from 0 to 3, as said below
Outputs:
- interferogram: float32 [2, 16, 512, 128], P(None, 'groups', 'az'), parts along dimension 1
- coherence: float32 [16, 512, 128], P('groups', 'az'), parts along dimension 0
The draws below stay inside these ranges and needn't reach their ends.
There are 4 independent parts, one for each index of `groups`. The reference program is written for one: setup_inputs(seed, part) draws one part's arguments, and reference() takes and returns one part's arrays. A program takes and returns all parts, laid end to end along the dimension named above; each array names one. Nothing has to cross between parts.
Inputs may be any that keep to these rules, and one draw needn't show every extreme that they name: `sweep_start_index`: the valid lines of burst b lie at merged rows from b * 40 - 15 to (b + 1) * 40 + 14, and some burst reaches both ends. The valid lines of all bursts together cover every merged row from 0 to 2559. `usable_azimuth_extent`: first below end for every burst. `usable_column_extent`: first below end for every burst. `image_couples`: the two acquisitions of a pair differ.
All inputs are finite; a program needn't handle non-finite values.
Results may differ from the reference program's by a relative error of at most 0.0003.
Values may be sent and summed in bfloat16 or wider, within the bound.
No kernel may reach another device: no remote copies, remote signals or barrier semaphores. Data moves between devices by JAX's collectives and lax.ppermute only.
A program may use at most 64 MiB of HBM per device.

```python
import math
import jax
import jax.numpy as jnp
from jax import lax

BLOCK_HEIGHT = 40
SLANT_WIDTH = 2560
IMAGE_TOTAL = 4
PAIRS = 4
LOOK_ROWS = 5
LOOK_COLS = 20
SHIFT_BOUND_MAX = 10
SPILL_REACH = 5
SWEEP_HEIGHT = 80
SWEEP_TOTAL = 64
GRID_HEIGHT = 2560


def geometry(key):
    seed_stream = jax.random.split(jax.random.fold_in(key, 7), 5)
    index_grid = jnp.arange(SWEEP_TOTAL + 1, dtype=jnp.int32)
    sweep_identifiers = jnp.arange(SWEEP_TOTAL, dtype=jnp.int32)
    edge_shifts = jax.random.randint(seed_stream[0], (SWEEP_TOTAL + 1,), 0 - SHIFT_BOUND_MAX, SHIFT_BOUND_MAX + 1, dtype=jnp.int32)
    peak_amount = jax.random.randint(seed_stream[1], (), 1, SWEEP_TOTAL - 1, dtype=jnp.int32)
    edge_shifts = jnp.where(index_grid == peak_amount, 0 - SHIFT_BOUND_MAX, edge_shifts)
    edge_shifts = jnp.where(index_grid == peak_amount + 1, SHIFT_BOUND_MAX, edge_shifts)
    edge_shifts = jnp.where((index_grid == 0) | (index_grid == SWEEP_TOTAL), 0, edge_shifts)
    sweep_edges = index_grid * BLOCK_HEIGHT + edge_shifts
    south_spill = jax.random.randint(seed_stream[2], (SWEEP_TOTAL,), 1, SPILL_REACH + 1, dtype=jnp.int32)
    south_spill = jnp.where(sweep_identifiers == peak_amount, SPILL_REACH, south_spill)
    north_spill = jax.random.randint(seed_stream[3], (SWEEP_TOTAL,), 1, SPILL_REACH + 1, dtype=jnp.int32)
    north_spill = jnp.where(sweep_identifiers == peak_amount, SPILL_REACH, north_spill)
    head_indices = jax.random.randint(seed_stream[4], (SWEEP_TOTAL,), 0, SPILL_REACH + 1, dtype=jnp.int32)
    start_indices = sweep_edges[:SWEEP_TOTAL] - south_spill - head_indices
    closing_indices = head_indices + south_spill + (sweep_edges[1:] - sweep_edges[:SWEEP_TOTAL]) + north_spill
    return (start_indices, head_indices, closing_indices)


def draw_sweep_start_index(key, part):
    return geometry(key)[0].astype(jnp.int32)


def draw_usable_azimuth_extent(key, part):
    start_indices, head_indices, closing_indices = geometry(key)
    return jnp.stack([head_indices, closing_indices], axis=1).astype(jnp.int32)


def draw_usable_column_extent(key, part):
    seed_stream = jax.random.split(jax.random.fold_in(key, 13), 2)
    least_index = jax.random.randint(seed_stream[0], (SWEEP_TOTAL,), 0, SLANT_WIDTH // 4, dtype=jnp.int32)
    cutoff_index = jax.random.randint(seed_stream[1], (SWEEP_TOTAL,), 0, SLANT_WIDTH // 4, dtype=jnp.int32)
    return jnp.stack([least_index, SLANT_WIDTH - cutoff_index], axis=1).astype(jnp.int32)


def draw_image_couples(key, part):
    seed_stream = jax.random.split(jax.random.fold_in(key, 17), 2)
    first_acq = jax.random.randint(seed_stream[0], (PAIRS,), 0, IMAGE_TOTAL, dtype=jnp.int32)
    step_acq = jax.random.randint(seed_stream[1], (PAIRS,), 1, IMAGE_TOTAL, dtype=jnp.int32)
    return jnp.stack([first_acq, (first_acq + step_acq) % IMAGE_TOTAL], axis=1).astype(jnp.int32)


def draw_sweep_stack(key, part):
    seed_stream = jax.random.split(jax.random.fold_in(key, 11), 4)
    result_dims = (2, IMAGE_TOTAL, SWEEP_TOTAL, SWEEP_HEIGHT, SLANT_WIDTH)
    common_indices = jax.random.normal(seed_stream[0], (2, 1, SWEEP_TOTAL, SWEEP_HEIGHT, SLANT_WIDTH), jnp.float32)
    single = jax.random.normal(seed_stream[1], result_dims, jnp.float32)
    mixture = 0.7 * (common_indices + single)
    azimuth_scale = jnp.exp(jax.random.uniform(seed_stream[2], (SWEEP_TOTAL, SWEEP_HEIGHT), jnp.float32, -0.7, 0.7))
    sample_scale = jnp.exp(jax.random.uniform(seed_stream[3], (SLANT_WIDTH,), jnp.float32, -0.7, 0.7))
    scaled = mixture * azimuth_scale[None, None, :, :, None] * sample_scale
    return scaled.astype(jnp.bfloat16)


def steps_of(stream_key, dims, pieces, smallest, top_value):
    factor_of = 1.0
    for position, parts in pieces:
        draws = jax.random.uniform(jax.random.fold_in(jax.random.fold_in(stream_key, 6), position), (parts,), jnp.float32, smallest / len(pieces), top_value / len(pieces))
        factor_of = factor_of * jnp.repeat(jnp.exp(draws), dims[position] // parts).reshape((-1,) + (1,) * (len(dims) - 1 - position))
    return factor_of


def setup_inputs(seed: int = 0, part: int = 0) -> dict:
    keys = jax.random.split(jax.random.key(seed), 7)
    part_splits = jax.random.split(jax.random.fold_in(keys[6], part), 7)
    sweep_stack = draw_sweep_stack(jax.random.fold_in(jax.random.fold_in(keys[6], part), 71), part)
    blend_curve = jnp.clip(jnp.exp(math.log(4.0) - 2.7725887 * jax.random.uniform(part_splits[1], (SWEEP_TOTAL, SWEEP_HEIGHT), jnp.float32) ** steps_of(part_splits[1], (SWEEP_TOTAL, SWEEP_HEIGHT), ((0, 64),), -0.2, 0.2)), 0.25, 4.0).astype(jnp.bfloat16)
    sweep_start_index = draw_sweep_start_index(jax.random.fold_in(jax.random.fold_in(keys[6], part), 71), part)
    usable_azimuth_extent = draw_usable_azimuth_extent(jax.random.fold_in(jax.random.fold_in(keys[6], part), 71), part)
    usable_column_extent = draw_usable_column_extent(jax.random.fold_in(jax.random.fold_in(keys[6], part), 71), part)
    image_couples = draw_image_couples(jax.random.fold_in(jax.random.fold_in(keys[6], part), 71), part)
    return dict(sweep_stack=sweep_stack, blend_curve=blend_curve, sweep_start_index=sweep_start_index, usable_azimuth_extent=usable_azimuth_extent, usable_column_extent=usable_column_extent, image_couples=image_couples)


def box_sums(values):
    shaped = values.reshape(values.shape[:-2] + (GRID_HEIGHT // LOOK_ROWS, LOOK_ROWS, SLANT_WIDTH // LOOK_COLS, LOOK_COLS))
    return jnp.sum(shaped, axis=(-3, -1))


def reference(sweep_stack, blend_curve, sweep_start_index, usable_azimuth_extent, usable_column_extent, image_couples):
    azimuth_index = jnp.arange(SWEEP_HEIGHT, dtype=jnp.int32)
    column_index = jnp.arange(SLANT_WIDTH, dtype=jnp.int32)
    reference_point = jnp.zeros((), jnp.int32)
    cross_term = jnp.zeros((2, IMAGE_TOTAL, GRID_HEIGHT + 2 * SWEEP_HEIGHT, SLANT_WIDTH), jnp.float32)
    intensity_norm = jnp.zeros((GRID_HEIGHT + 2 * SWEEP_HEIGHT,), jnp.float32)

    def deposit_sweep(sweep_index, cumulative_sums):
        aggregate, blend_total = cumulative_sums
        sweep_content = lax.dynamic_index_in_dim(sweep_stack, sweep_index, 2, keepdims=False)
        usable_marks = (azimuth_index >= usable_azimuth_extent[sweep_index, 0]) & (azimuth_index < usable_azimuth_extent[sweep_index, 1])
        azimuth_blend = jnp.where(usable_marks, blend_curve[sweep_index], jnp.zeros((), jnp.bfloat16)).astype(jnp.float32)
        column_usable = ((column_index >= usable_column_extent[sweep_index, 0]) & (column_index < usable_column_extent[sweep_index, 1])).astype(jnp.float32)
        added_term = sweep_content.astype(jnp.float32) * azimuth_blend[:, None] * column_usable[None, :]
        start_index = (sweep_start_index[sweep_index] + SWEEP_HEIGHT).astype(jnp.int32)
        available = lax.dynamic_slice(aggregate, (reference_point, reference_point, start_index, reference_point), (2, IMAGE_TOTAL, SWEEP_HEIGHT, SLANT_WIDTH))
        aggregate = lax.dynamic_update_slice(aggregate, available + added_term, (reference_point, reference_point, start_index, reference_point))
        available_blends = lax.dynamic_slice(blend_total, (start_index,), (SWEEP_HEIGHT,))
        blend_total = lax.dynamic_update_slice(blend_total, available_blends + azimuth_blend, (start_index,))
        return aggregate, blend_total

    cross_term, intensity_norm = lax.fori_loop(0, SWEEP_TOTAL, deposit_sweep, (cross_term, intensity_norm))
    combined_grid = cross_term[:, :, SWEEP_HEIGHT:SWEEP_HEIGHT + GRID_HEIGHT] / intensity_norm[SWEEP_HEIGHT:SWEEP_HEIGHT + GRID_HEIGHT][:, None]
    intensity = combined_grid[0] * combined_grid[0] + combined_grid[1] * combined_grid[1]
    first_image = jnp.take(combined_grid, image_couples[:, 0], axis=1)
    second_image = jnp.take(combined_grid, image_couples[:, 1], axis=1)
    real_part = first_image[0] * second_image[0] + first_image[1] * second_image[1]
    imag_part = first_image[1] * second_image[0] - first_image[0] * second_image[1]
    look_sum = box_sums(jnp.stack([real_part, imag_part]))
    look_power = box_sums(intensity)
    power_first = jnp.take(look_power, image_couples[:, 0], axis=0)
    power_second = jnp.take(look_power, image_couples[:, 1], axis=0)
    coherence = (look_sum[0] * look_sum[0] + look_sum[1] * look_sum[1]) / jnp.maximum(power_first * power_second, 1.0)
    interferogram = look_sum / (LOOK_ROWS * LOOK_COLS)
    return interferogram, coherence
```

```python
import jax
import jax.numpy as jnp
from jax import lax
from jax.experimental import pallas as pl
from jax.experimental.pallas import tpu as pltpu
from jax.sharding import PartitionSpec as P

BLOCK_HEIGHT = 40
SLANT_WIDTH = 2560
LOOK_ROWS = 5
LOOK_COLS = 20
MARGIN = 15
SWEEP_HEIGHT = 80
IMAGES = 4
PLANES = 2 * IMAGES
PAIRS = 4
SENT = 16
WINDOW = 32
LOOKS = SLANT_WIDTH // LOOK_COLS
BOXES = BLOCK_HEIGHT // LOOK_ROWS
TILE = 256
TILES = SLANT_WIDTH // TILE
F32 = jnp.float32
BF16 = jnp.bfloat16

HBM = pl.BlockSpec(memory_space=pltpu.HBM)
VMEM = pl.BlockSpec(memory_space=pltpu.VMEM)
SMEM = pl.BlockSpec(memory_space=pltpu.SMEM)


def iota(shape, dim):
    return lax.broadcasted_iota(jnp.int32, shape, dim)


def line_offset(start_ref):
    return lax.axis_index("az") * BLOCK_HEIGHT - start_ref[0]


def pack_kernel(start_ref, lines_ref, cols_ref, curve_ref, x_ref, a_ref, b_ref, win, sems):
    az = lax.axis_index("az")
    odd = lax.rem(az, 2)
    offset = line_offset(start_ref)
    down = offset - MARGIN
    up = offset + BLOCK_HEIGHT
    firsts = (jnp.where(odd == 1, down, up), jnp.where(odd == 1, up, down))
    copies = []
    bases = []
    for side in range(2):
        base = jnp.clip(
            lax.shift_left(lax.shift_right_arithmetic(firsts[side], 4), 4),
            0,
            SWEEP_HEIGHT - WINDOW,
        )
        base = pl.multiple_of(base, 16)
        bases.append(base)
        for p in range(PLANES):
            copy = pltpu.make_async_copy(
                x_ref.at[p // IMAGES, p % IMAGES, 0, pl.ds(base, WINDOW), :],
                win.at[side, p],
                sems.at[side, p],
            )
            copy.start()
            copies.append(copy)
    first_line, end_line = lines_ref[0, 0], lines_ref[0, 1]
    first_col, end_col = cols_ref[0, 0], cols_ref[0, 1]
    col = iota((1, SLANT_WIDTH), 1)
    inside = ((col >= first_col) & (col < end_col)).astype(F32).astype(BF16)
    curve = jnp.broadcast_to(curve_ref[...], (SENT, SWEEP_HEIGHT))
    outs = (a_ref, b_ref)
    for side in range(2):
        start = firsts[side]
        line = iota((SWEEP_HEIGHT, 128), 0)
        place = iota((SWEEP_HEIGHT, 128), 1)
        chosen = (
            (line == start + place)
            & (place < MARGIN)
            & (line >= first_line)
            & (line < end_line)
        )
        weights = jnp.dot(
            curve, chosen.astype(F32).astype(BF16), preferred_element_type=F32
        ).astype(BF16)
        row = iota((SENT, WINDOW), 0)
        source = iota((SENT, WINDOW), 1) + bases[side]
        pick = ((source == start + row) & (row < MARGIN)).astype(F32).astype(BF16)
        for p in range(PLANES):
            copies[side * PLANES + p].wait()
            for t in range(TILES):
                cols = slice(t * TILE, (t + 1) * TILE)
                block = jnp.dot(
                    pick, win[side, p, :, cols], preferred_element_type=F32
                ).astype(BF16)
                outs[side][p, :, cols] = block * inside[:, cols]
        head = outs[side][0, :, :128]
        last = iota((SENT, 128), 0) == MARGIN
        outs[side][0, :, :128] = jnp.where(last, weights, head)


def merge_kernel(
    start_ref,
    lines_ref,
    cols_ref,
    couples_ref,
    curve_ref,
    x_ref,
    a_ref,
    b_ref,
    ifg_ref,
    coh_ref,
    merged,
    acc,
    power,
):
    az = lax.axis_index("az")
    odd = lax.rem(az, 2)
    offset = line_offset(start_ref)
    slot = iota((BLOCK_HEIGHT, SWEEP_HEIGHT), 0)
    row = (slot & 7) * LOOK_ROWS + (slot >> 3)
    line = iota((BLOCK_HEIGHT, SWEEP_HEIGHT), 1)
    own = (line == row + offset) & (line >= lines_ref[0, 0]) & (line < lines_ref[0, 1])
    own = jnp.where(own, curve_ref[...].astype(F32), 0.0)

    def partner(ref, base):
        slot = iota((BLOCK_HEIGHT, SENT), 0)
        row = (slot & 7) * LOOK_ROWS + (slot >> 3)
        place = iota((BLOCK_HEIGHT, SENT), 1)
        weights = ref[0, MARGIN:SENT, :SENT].astype(F32)
        return jnp.where((row == base + place) & (place < MARGIN), weights, 0.0)

    above = BLOCK_HEIGHT - MARGIN
    side_a = partner(a_ref, jnp.where(odd == 1, 0, above))
    side_b = partner(b_ref, jnp.where(odd == 1, above, 0))
    select = jnp.concatenate([own, side_a, side_b], axis=1)
    total = jnp.sum(select, axis=1, keepdims=True)
    scale = jnp.broadcast_to(1.0 / total, (BLOCK_HEIGHT, TILE))
    select = select.astype(BF16)
    first_col, end_col = cols_ref[0, 0], cols_ref[0, 1]
    acc[...] = jnp.zeros_like(acc)

    def tile(t, carry):
        cols = pl.ds(pl.multiple_of(t * TILE, TILE), TILE)
        col = iota((1, TILE), 1) + t * TILE
        inside = ((col >= first_col) & (col < end_col)).astype(F32).astype(BF16)
        for p in range(PLANES):
            values = jnp.concatenate(
                [
                    x_ref[p // IMAGES, p % IMAGES, 0, :, cols] * inside,
                    a_ref[p, :, cols],
                    b_ref[p, :, cols],
                ],
                axis=0,
            )
            merged[p // IMAGES, p % IMAGES] = (
                jnp.dot(select, values, preferred_element_type=F32) * scale
            )

        def rows(v):
            return jnp.sum(v.reshape(LOOK_ROWS, BOXES, TILE), axis=0)

        real, imag, powers = [], [], []
        for p in range(PAIRS):
            i, j = couples_ref[p, 0], couples_ref[p, 1]
            ri, ii, rj, ij = merged[0, i], merged[1, i], merged[0, j], merged[1, j]
            real.append(rows(ri * rj + ii * ij))
            imag.append(rows(ii * rj - ri * ij))
        for a in range(IMAGES):
            powers.append(rows(merged[0, a] * merged[0, a] + merged[1, a] * merged[1, a]))
        sums = jnp.concatenate(real + imag + powers, axis=0)
        high = sums.astype(BF16)
        low = (sums - high.astype(F32)).astype(BF16)
        where = iota((TILE, LOOKS), 0) + t * TILE
        look = iota((TILE, LOOKS), 1) * LOOK_COLS
        box = ((where >= look) & (where < look + LOOK_COLS)).astype(F32).astype(BF16)
        acc[...] += jnp.dot(high, box, preferred_element_type=F32) + jnp.dot(
            low, box, preferred_element_type=F32
        )
        return carry

    lax.fori_loop(0, TILES, tile, 0)
    for a in range(IMAGES):
        power[a] = acc[(2 * PAIRS + a) * BOXES : (2 * PAIRS + a + 1) * BOXES, :]
    for p in range(PAIRS):
        re = acc[p * BOXES : (p + 1) * BOXES, :]
        im = acc[(PAIRS + p) * BOXES : (PAIRS + p + 1) * BOXES, :]
        ifg_ref[0, p] = re / float(LOOK_ROWS * LOOK_COLS)
        ifg_ref[1, p] = im / float(LOOK_ROWS * LOOK_COLS)
        both = power[couples_ref[p, 0]] * power[couples_ref[p, 1]]
        coh_ref[p] = (re * re + im * im) / jnp.maximum(both, 1.0)


def swaps(n, first):
    pairs = [(k, k + 1) for k in range(first, n - 1, 2)]
    return pairs + [(j, i) for i, j in pairs]


def per_device(
    sweep_stack,
    blend_curve,
    sweep_start_index,
    usable_azimuth_extent,
    usable_column_extent,
    image_couples,
):
    n = lax.axis_size("az")
    sent = pltpu.VMEM((PLANES, SENT, SLANT_WIDTH), BF16)
    in_hbm = pltpu.with_memory_space_constraint(sweep_stack, pltpu.HBM)
    to_a, to_b = pl.pallas_call(
        pack_kernel,
        out_shape=(sent, sent),
        in_specs=[SMEM, SMEM, SMEM, VMEM, HBM],
        out_specs=(VMEM, VMEM),
        scratch_shapes=[
            pltpu.VMEM((2, PLANES, WINDOW, SLANT_WIDTH), BF16),
            pltpu.SemaphoreType.DMA((2, PLANES)),
        ],
        compiler_params=pltpu.CompilerParams(vmem_limit_bytes=16 * 2**20),
        name="pack",
    )(sweep_start_index, usable_azimuth_extent, usable_column_extent, blend_curve, in_hbm)
    from_b = lax.ppermute(to_b, "az", swaps(n, 1))
    from_a = lax.ppermute(to_a, "az", swaps(n, 0))
    from_a = pltpu.with_memory_space_constraint(from_a, pltpu.VMEM)
    from_b = pltpu.with_memory_space_constraint(from_b, pltpu.VMEM)
    return pl.pallas_call(
        merge_kernel,
        out_shape=(
            jax.ShapeDtypeStruct((2, PAIRS, BOXES, LOOKS), F32),
            jax.ShapeDtypeStruct((PAIRS, BOXES, LOOKS), F32),
        ),
        in_specs=[SMEM, SMEM, SMEM, SMEM, VMEM, VMEM, VMEM, VMEM],
        out_specs=(VMEM, VMEM),
        scratch_shapes=[
            pltpu.VMEM((2, IMAGES, BLOCK_HEIGHT, TILE), F32),
            pltpu.VMEM((3 * PAIRS * BOXES, LOOKS), F32),
            pltpu.VMEM((IMAGES, BOXES, LOOKS), F32),
        ],
        compiler_params=pltpu.CompilerParams(vmem_limit_bytes=16 * 2**20),
        name="merge",
    )(
        sweep_start_index,
        usable_azimuth_extent,
        usable_column_extent,
        image_couples,
        blend_curve,
        sweep_stack,
        from_a,
        from_b,
    )


def solution(mesh):
    return jax.shard_map(
        per_device,
        mesh=mesh,
        in_specs=(
            P(None, None, ("groups", "az"), None, None),
            P(("groups", "az"), None),
            P(("groups", "az")),
            P(("groups", "az"), None),
            P(("groups", "az"), None),
            P("groups", None),
        ),
        out_specs=(P(None, "groups", "az", None), P("groups", "az", None)),
        check_vma=False,
    )
```

```python
import functools

import jax
import jax.numpy as jnp
from jax import lax
from jax.experimental import pallas as pl
from jax.experimental.pallas import tpu as pltpu
from jax.sharding import PartitionSpec as P

BLOCK_HEIGHT = 40
SLANT_WIDTH = 2560
LOOK_ROWS = 5
LOOK_COLS = 20
MARGIN = 15
SWEEP_HEIGHT = 80
IMAGES = 4
PLANES = 2 * IMAGES
PAIRS = 4
SENT = 16
WINDOW = 32
LOOKS = SLANT_WIDTH // LOOK_COLS
BOXES = BLOCK_HEIGHT // LOOK_ROWS
EDGE_BOXES = MARGIN // LOOK_ROWS
SUMS = (2 * PAIRS + IMAGES) * BOXES
TILE = 256
TILES = SLANT_WIDTH // TILE
HALF = SLANT_WIDTH // 2
F32 = jnp.float32
BF16 = jnp.bfloat16

HBM = pl.BlockSpec(memory_space=pltpu.HBM)
VMEM = pl.BlockSpec(memory_space=pltpu.VMEM)
SMEM = pl.BlockSpec(memory_space=pltpu.SMEM)


def iota(shape, dim):
    return lax.broadcasted_iota(jnp.int32, shape, dim)


def as_bf16(mask):
    return mask.astype(F32).astype(BF16)


def position():
    az = lax.axis_index("az")
    return az, lax.rem(az, 2) == 1


def columns_inside(cols_ref, first, count):
    col = iota((1, count), 1) + first
    return as_bf16((col >= cols_ref[0, 0]) & (col < cols_ref[0, 1]))


def take_lines(first, x_plane, lines_ref, cols_ref, curve_ref, out_ref):
    base = lax.shift_left(lax.shift_right_arithmetic(first, 4), 4)
    base = pl.multiple_of(jnp.clip(base, 0, SWEEP_HEIGHT - WINDOW), 16)
    line = iota((SWEEP_HEIGHT, 128), 0)
    place = iota((SWEEP_HEIGHT, 128), 1)
    chosen = (
        (line == first + place)
        & (place < MARGIN)
        & (line >= lines_ref[0, 0])
        & (line < lines_ref[0, 1])
    )
    curve = jnp.broadcast_to(curve_ref[...], (SENT, SWEEP_HEIGHT))
    weights = jnp.dot(curve, as_bf16(chosen), preferred_element_type=F32).astype(BF16)
    row = iota((SENT, WINDOW), 0)
    source = iota((SENT, WINDOW), 1) + base
    pick = as_bf16((source == first + row) & (row < MARGIN))
    inside = columns_inside(cols_ref, 0, SLANT_WIDTH)
    for p in range(PLANES):
        window = x_plane(p)
        for t in range(TILES):
            cols = slice(t * TILE, (t + 1) * TILE)
            block = jnp.dot(pick, window[pl.ds(base, WINDOW), cols], preferred_element_type=F32)
            out_ref[p, :, cols] = block.astype(BF16) * inside[:, cols]
    last = iota((SENT, 128), 0) == MARGIN
    out_ref[0, :, :128] = jnp.where(last, weights, out_ref[0, :, :128])


def pack_kernel(
    start_ref,
    lines_hbm,
    cols_hbm,
    curve_hbm,
    x_hbm,
    a_ref,
    b_ref,
    x,
    lines_ref,
    cols_ref,
    curve_ref,
    sems,
    small_sems,
):
    small = (
        pltpu.make_async_copy(lines_hbm, lines_ref, small_sems.at[0]),
        pltpu.make_async_copy(cols_hbm, cols_ref, small_sems.at[1]),
        pltpu.make_async_copy(curve_hbm, curve_ref, small_sems.at[2]),
    )
    for copy in small:
        copy.start()
    planes = [
        pltpu.make_async_copy(x_hbm.at[p // IMAGES, p % IMAGES, 0], x.at[p], sems.at[p])
        for p in range(PLANES)
    ]
    for copy in planes:
        copy.start()
    for copy in small:
        copy.wait()
    az, odd = position()
    offset = az * BLOCK_HEIGHT - start_ref[0]
    down = offset - MARGIN
    up = offset + BLOCK_HEIGHT

    def arriving(p):
        planes[p].wait()
        return x.at[p]

    take_lines(jnp.where(odd, down, up), arriving, lines_ref, cols_ref, curve_ref, a_ref)

    @pl.when((az > 0) & (az < lax.axis_size("az") - 1))
    def _():
        take_lines(jnp.where(odd, up, down), x.at.__getitem__, lines_ref, cols_ref, curve_ref, b_ref)


def reciprocal(total):
    return jnp.where(total > 0.0, 1.0 / total, 0.0)


def look_sums(merged, couples_ref, box):
    def rows(v):
        return jnp.sum(v.reshape(LOOK_ROWS, BOXES, TILE), axis=0)

    real, imag, powers = [], [], []
    for p in range(PAIRS):
        i, j = couples_ref[p, 0], couples_ref[p, 1]
        ri, ii, rj, ij = merged[0, i], merged[1, i], merged[0, j], merged[1, j]
        real.append(rows(ri * rj + ii * ij))
        imag.append(rows(ii * rj - ri * ij))
    for a in range(IMAGES):
        re, im = merged[0, a], merged[1, a]
        powers.append(rows(re * re + im * im))
    sums = jnp.concatenate(real + imag + powers, axis=0)
    high = sums.astype(BF16)
    low = (sums - high.astype(F32)).astype(BF16)
    return jnp.dot(high, box, preferred_element_type=F32) + jnp.dot(
        low, box, preferred_element_type=F32
    )


def look_box(first):
    where = iota((TILE, LOOKS), 0) + first
    look = iota((TILE, LOOKS), 1) * LOOK_COLS
    return as_bf16((where >= look) & (where < look + LOOK_COLS))


def partner_weights(ref):
    return ref[0, MARGIN:SENT, :SENT].astype(F32)


def own_kernel(
    late,
    start_ref,
    lines_ref,
    cols_ref,
    couples_ref,
    curve_ref,
    x_hbm,
    b_ref,
    *rest,
):
    lines_out, sums_out, x, merged, sem = rest[-5:]
    az, odd = position()

    @pl.when((az == 0) if late else (az > 0))
    def _():
        copy = pltpu.make_async_copy(x_hbm, x, sem)
        copy.start()
        copy.wait()
        offset = az * BLOCK_HEIGHT - start_ref[0]
        above = BLOCK_HEIGHT - MARGIN
        first = offset + jnp.where(odd, 0, above)
        take_lines(
            first,
            lambda p: x.at[p // IMAGES, p % IMAGES, 0],
            lines_ref,
            cols_ref,
            curve_ref,
            lines_out,
        )
        slot = iota((BLOCK_HEIGHT, SWEEP_HEIGHT), 0)
        row = (slot & 7) * LOOK_ROWS + (slot >> 3)
        line = iota((BLOCK_HEIGHT, SWEEP_HEIGHT), 1)
        own = (line == row + offset) & (line >= lines_ref[0, 0]) & (line < lines_ref[0, 1])
        own = jnp.where(own, curve_ref[...].astype(F32), 0.0)
        slot = iota((BLOCK_HEIGHT, SENT), 0)
        row = (slot & 7) * LOOK_ROWS + (slot >> 3)
        place = iota((BLOCK_HEIGHT, SENT), 1)
        match = (row == place + jnp.where(odd, above, 0)) & (place < MARGIN)
        other = jnp.where(match, partner_weights(b_ref), 0.0)
        select = jnp.concatenate([own, other], axis=1)
        total = jnp.sum(select, axis=1, keepdims=True)
        scale = jnp.broadcast_to(reciprocal(total), (BLOCK_HEIGHT, TILE))
        select = select.astype(BF16)
        sums_out[...] = jnp.zeros_like(sums_out)

        def two_tiles(k, carry):
            for u in range(2):
                begin = pl.multiple_of((k * 2 + u) * TILE, TILE)
                cols = pl.ds(begin, TILE)
                inside = columns_inside(cols_ref, begin, TILE)
                for p in range(PLANES):
                    c, a = p // IMAGES, p % IMAGES
                    values = jnp.concatenate(
                        [x[c, a, 0, :, cols] * inside, b_ref[p, :, cols]], axis=0
                    )
                    merged[u, c, a] = (
                        jnp.dot(select, values, preferred_element_type=F32) * scale
                    )
            sums = [
                look_sums(merged.at[u], couples_ref, look_box((k * 2 + u) * TILE))
                for u in range(2)
            ]
            sums_out[...] += sums[0] + sums[1]
            return carry

        lax.fori_loop(0, TILES // 2, two_tiles, 0)


def edge_kernel(couples_ref, a_ref, own_ref, sums_ref, ifg_ref, coh_ref, merged, acc, power):
    _, odd = position()
    slot = iota((BLOCK_HEIGHT, SENT), 0)
    place = iota((BLOCK_HEIGHT, SENT), 1)
    edge = slot & 3
    match = (place == edge * LOOK_ROWS + (slot >> 3)) & (edge < EDGE_BOXES)
    lower = (slot & 4) == 0
    theirs = jnp.where(match, partner_weights(a_ref), 0.0)
    ours = jnp.where(match, partner_weights(own_ref), 0.0)
    total = jnp.sum(theirs + ours, axis=1, keepdims=True)
    scale = jnp.broadcast_to(reciprocal(total), (BLOCK_HEIGHT, TILE))
    select = jnp.concatenate(
        [
            jnp.where(lower, theirs, 0.0),
            jnp.where(lower, ours, 0.0),
            jnp.where(lower, 0.0, theirs),
            jnp.where(lower, 0.0, ours),
        ],
        axis=1,
    ).astype(BF16)
    total = None
    for t in range(HALF // TILE):
        one = slice(t * TILE, (t + 1) * TILE)
        two = slice(HALF + t * TILE, HALF + (t + 1) * TILE)
        for p in range(PLANES):
            values = jnp.concatenate(
                [a_ref[p, :, one], own_ref[p, :, one], a_ref[p, :, two], own_ref[p, :, two]],
                axis=0,
            )
            merged[t, p // IMAGES, p % IMAGES] = (
                jnp.dot(select, values, preferred_element_type=F32) * scale
            )
        part = look_sums(merged.at[t], couples_ref, look_box(t * TILE))
        total = part if total is None else total + part
    acc[...] = total
    sublane = iota((BOXES, LOOKS), 0)
    lane = iota((BOXES, LOOKS), 1)
    lowest = jnp.where(odd, 0, BOXES - EDGE_BOXES)
    mine = (sublane >= lowest) & (sublane < lowest + EDGE_BOXES)

    def whole(u):
        part = acc[u * BOXES : (u + 1) * BOXES, :]
        upper = pltpu.roll(pltpu.roll(part, LOOKS // 2, 1), 4, 0)
        part = jnp.where(lane < LOOKS // 2, part, upper)
        part = jnp.where(odd, part, pltpu.roll(part, BOXES - EDGE_BOXES, 0))
        return jnp.where(mine, part, sums_ref[u * BOXES : (u + 1) * BOXES, :])

    for a in range(IMAGES):
        power[a] = whole(2 * PAIRS + a)
    for p in range(PAIRS):
        re = whole(p)
        im = whole(PAIRS + p)
        ifg_ref[0, p] = re / float(LOOK_ROWS * LOOK_COLS)
        ifg_ref[1, p] = im / float(LOOK_ROWS * LOOK_COLS)
        both = power[couples_ref[p, 0]] * power[couples_ref[p, 1]]
        coh_ref[p] = (re * re + im * im) / jnp.maximum(both, 1.0)


def swaps(n, first):
    pairs = [(k, k + 1) for k in range(first, n - 1, 2)]
    return pairs + [(j, i) for i, j in pairs]


def limit(mebibytes):
    return pltpu.CompilerParams(vmem_limit_bytes=mebibytes * 2**20)


def in_hbm(array):
    return pltpu.with_memory_space_constraint(array, pltpu.HBM)


def per_device(
    sweep_stack,
    blend_curve,
    sweep_start_index,
    usable_azimuth_extent,
    usable_column_extent,
    image_couples,
):
    n = lax.axis_size("az")
    sent = jax.ShapeDtypeStruct((PLANES, SENT, SLANT_WIDTH), BF16)
    small = (sweep_start_index, usable_azimuth_extent, usable_column_extent)
    to_a, to_b = pl.pallas_call(
        pack_kernel,
        out_shape=(sent, sent),
        in_specs=[SMEM] + [HBM] * 4,
        out_specs=(VMEM, VMEM),
        scratch_shapes=[
            pltpu.VMEM((PLANES, SWEEP_HEIGHT, SLANT_WIDTH), BF16),
            pltpu.SMEM((1, 2), jnp.int32),
            pltpu.SMEM((1, 2), jnp.int32),
            pltpu.VMEM((1, SWEEP_HEIGHT), BF16),
            pltpu.SemaphoreType.DMA((PLANES,)),
            pltpu.SemaphoreType.DMA((3,)),
        ],
        compiler_params=limit(16),
        name="pack",
    )(small[0], *(in_hbm(array) for array in (*small[1:], blend_curve, sweep_stack)))
    from_b = lax.ppermute(to_b, "az", swaps(n, 1))
    from_a = lax.ppermute(to_a, "az", swaps(n, 0))

    def own(late, *before):
        operands = (*small, image_couples, blend_curve, in_hbm(sweep_stack), from_b, *before)
        return pl.pallas_call(
            functools.partial(own_kernel, late),
            out_shape=(sent, jax.ShapeDtypeStruct((SUMS, LOOKS), F32)),
            in_specs=[SMEM] * 4 + [VMEM, HBM, VMEM] + [VMEM] * len(before),
            out_specs=(VMEM, VMEM),
            scratch_shapes=[
                pltpu.VMEM((2, IMAGES, 1, SWEEP_HEIGHT, SLANT_WIDTH), BF16),
                pltpu.VMEM((2, 2, IMAGES, BLOCK_HEIGHT, TILE), F32),
                pltpu.SemaphoreType.DMA,
            ],
            input_output_aliases={7: 0, 8: 1} if before else {},
            compiler_params=limit(16),
            name="late" if late else "early",
        )(*operands)

    lines, sums = own(False)
    lines, sums = own(True, lines, sums)
    return pl.pallas_call(
        edge_kernel,
        out_shape=(
            jax.ShapeDtypeStruct((2, PAIRS, BOXES, LOOKS), F32),
            jax.ShapeDtypeStruct((PAIRS, BOXES, LOOKS), F32),
        ),
        in_specs=[SMEM, VMEM, VMEM, VMEM],
        out_specs=(VMEM, VMEM),
        scratch_shapes=[
            pltpu.VMEM((HALF // TILE, 2, IMAGES, BLOCK_HEIGHT, TILE), F32),
            pltpu.VMEM((SUMS, LOOKS), F32),
            pltpu.VMEM((IMAGES, BOXES, LOOKS), F32),
        ],
        compiler_params=limit(16),
        name="edge",
    )(image_couples, from_a, lines, sums)


def solution(mesh):
    return jax.shard_map(
        per_device,
        mesh=mesh,
        in_specs=(
            P(None, None, ("groups", "az"), None, None),
            P(("groups", "az"), None),
            P(("groups", "az")),
            P(("groups", "az"), None),
            P(("groups", "az"), None),
            P("groups", None),
        ),
        out_specs=(P(None, "groups", "az", None), P("groups", "az", None)),
        check_vma=False,
    )
```

```python
import functools

import jax
import jax.numpy as jnp
from jax import lax
from jax.experimental import pallas as pl
from jax.experimental.pallas import tpu as pltpu
from jax.sharding import PartitionSpec as P

BLOCK_HEIGHT = 40
SLANT_WIDTH = 2560
LOOK_ROWS = 5
LOOK_COLS = 20
MARGIN = 15
SWEEP_HEIGHT = 80
IMAGES = 4
PLANES = 2 * IMAGES
PAIRS = 4
SENT = 16
WINDOW = 32
LOOKS = SLANT_WIDTH // LOOK_COLS
BOXES = BLOCK_HEIGHT // LOOK_ROWS
TILE = 256
TILES = SLANT_WIDTH // TILE
F32 = jnp.float32
BF16 = jnp.bfloat16

HBM = pl.BlockSpec(memory_space=pltpu.HBM)
VMEM = pl.BlockSpec(memory_space=pltpu.VMEM)
SMEM = pl.BlockSpec(memory_space=pltpu.SMEM)


def iota(shape, dim):
    return lax.broadcasted_iota(jnp.int32, shape, dim)


def as_bf16(mask):
    return mask.astype(F32).astype(BF16)


def position():
    az = lax.axis_index("az")
    return az, lax.rem(az, 2) == 1


def columns_inside(cols_ref, first, count):
    col = iota((1, count), 1) + first
    return as_bf16((col >= cols_ref[0, 0]) & (col < cols_ref[0, 1]))


def window_base(first):
    base = lax.shift_left(lax.shift_right_arithmetic(first, 4), 4)
    return pl.multiple_of(jnp.clip(base, 0, SWEEP_HEIGHT - WINDOW), 16)


def take_lines(first, base, window, lines_ref, cols_ref, curve_ref, out_ref):
    line = iota((SWEEP_HEIGHT, 128), 0)
    place = iota((SWEEP_HEIGHT, 128), 1)
    chosen = (
        (line == first + place)
        & (place < MARGIN)
        & (line >= lines_ref[0, 0])
        & (line < lines_ref[0, 1])
    )
    curve = jnp.broadcast_to(curve_ref[...], (SENT, SWEEP_HEIGHT))
    weights = jnp.dot(curve, as_bf16(chosen), preferred_element_type=F32).astype(BF16)
    row = iota((SENT, WINDOW), 0)
    source = iota((SENT, WINDOW), 1) + base
    pick = as_bf16((source == first + row) & (row < MARGIN))
    inside = columns_inside(cols_ref, 0, SLANT_WIDTH)
    for p in range(PLANES):
        lines = window(p)
        for t in range(TILES):
            cols = slice(t * TILE, (t + 1) * TILE)
            block = jnp.dot(pick, lines[:, cols], preferred_element_type=F32)
            out_ref[p, :, cols] = block.astype(BF16) * inside[:, cols]
    last = iota((SENT, 128), 0) == MARGIN
    out_ref[0, :, :128] = jnp.where(last, weights, out_ref[0, :, :128])


def start_all(*pairs):
    copies = [pltpu.make_async_copy(source, target, sem) for source, target, sem in pairs]
    for copy in copies:
        copy.start()
    return copies


def wait_all(copies):
    for copy in copies:
        copy.wait()


def pack_kernel(
    start_ref,
    lines_hbm,
    cols_hbm,
    curve_hbm,
    x_hbm,
    a_ref,
    b_ref,
    windows,
    lines_ref,
    cols_ref,
    curve_ref,
    sems,
    small_sems,
):
    az, odd = position()
    offset = az * BLOCK_HEIGHT - start_ref[0]
    down = offset - MARGIN
    up = offset + BLOCK_HEIGHT
    firsts = (jnp.where(odd, down, up), jnp.where(odd, up, down))
    bases = [window_base(first) for first in firsts]

    def fetch(side):
        rows = pl.ds(bases[side], WINDOW)
        return start_all(
            *(
                (
                    x_hbm.at[p // IMAGES, p % IMAGES, 0, rows, :],
                    windows.at[side, p],
                    sems.at[side, p],
                )
                for p in range(PLANES)
            )
        )

    near = fetch(0)
    small = start_all(
        (lines_hbm, lines_ref, small_sems.at[0]),
        (cols_hbm, cols_ref, small_sems.at[1]),
        (curve_hbm, curve_ref, small_sems.at[2]),
    )
    wait_all(small)

    def take(side, copies, out_ref):
        def window(p):
            copies[p].wait()
            return windows.at[side, p]

        take_lines(firsts[side], bases[side], window, lines_ref, cols_ref, curve_ref, out_ref)

    take(0, near, a_ref)

    @pl.when((az > 0) & (az < lax.axis_size("az") - 1))
    def _():
        take(1, fetch(1), b_ref)


def weights_of(ref):
    return ref[0, MARGIN:SENT, :SENT].astype(F32)


def box_sums(parts, boxes, sources, couples_ref, merged_refs, ready=None):
    stride = BOXES // parts
    width = SLANT_WIDTH // parts
    slot = iota((BLOCK_HEIGHT, SENT), 0)
    place = iota((BLOCK_HEIGHT, SENT), 1)
    box = slot & (stride - 1)
    part = (slot & 7) // stride
    match = (place == box * LOOK_ROWS + (slot >> 3)) & (box < boxes)
    chosen = [jnp.where(match, weights_of(ref), 0.0) for ref in sources]
    total = jnp.sum(sum(chosen), axis=1, keepdims=True)
    scale = jnp.where(total > 0.0, 1.0 / total, 0.0)
    scale = jnp.broadcast_to(scale, (BLOCK_HEIGHT, TILE))
    select = jnp.concatenate(
        [jnp.where(part == q, w, 0.0) for q in range(parts) for w in chosen], axis=1
    ).astype(BF16)
    tiles = [(at, min(TILE, width - at)) for at in range(0, width, TILE)]
    for (at, size), merged in zip(tiles, merged_refs):
        for p in range(PLANES):
            values = jnp.concatenate(
                [
                    ref[p, :, q * width + at : q * width + at + size]
                    for q in range(parts)
                    for ref in sources
                ],
                axis=0,
            )
            merged[p // IMAGES, p % IMAGES, :, :size] = (
                jnp.dot(select, values, preferred_element_type=F32) * scale[:, :size]
            )
    if ready is not None:
        ready()
    couples = [(couples_ref[p, 0], couples_ref[p, 1]) for p in range(PAIRS)]
    acc = None
    for (at, size), merged in zip(tiles, merged_refs):

        def rows(v):
            return jnp.sum(v.reshape(LOOK_ROWS, BOXES, size), axis=0)

        def plane(c, image):
            return merged[c, image, :, :size]

        real, imag, powers = [], [], []
        for i, j in couples:
            ri, ii, rj, ij = plane(0, i), plane(1, i), plane(0, j), plane(1, j)
            real.append(rows(ri * rj + ii * ij))
            imag.append(rows(ii * rj - ri * ij))
        for a in range(IMAGES):
            re, im = plane(0, a), plane(1, a)
            powers.append(rows(re * re + im * im))
        sums = jnp.concatenate(real + imag + powers, axis=0)
        high = sums.astype(BF16)
        low = (sums - high.astype(F32)).astype(BF16)
        where = iota((size, LOOKS), 0) + at
        look = iota((size, LOOKS), 1) * LOOK_COLS
        cells = as_bf16((where >= look) & (where < look + LOOK_COLS))
        got = jnp.dot(high, cells, preferred_element_type=F32) + jnp.dot(
            low, cells, preferred_element_type=F32
        )
        acc = got if acc is None else acc + got
    lane = iota((BOXES, LOOKS), 1)
    step = LOOKS // parts
    out = []
    for u in range(3 * PAIRS):
        got = acc[u * BOXES : (u + 1) * BOXES, :]
        whole = got
        for q in range(1, parts):
            moved = pltpu.roll(pltpu.roll(got, q * step, 1), BOXES - q * stride, 0)
            whole = jnp.where(lane >= q * step, moved, whole)
        out.append(whole)
    return out


def own_kernel(
    late,
    start_ref,
    lines_hbm,
    cols_hbm,
    couples_hbm,
    curve_hbm,
    x_hbm,
    *rest,
):
    (
        a_out,
        b_out,
        sums_out,
        x,
        middle,
        lines_ref,
        cols_ref,
        couples_ref,
        curve_ref,
        *merged,
        small_sems,
        sems,
    ) = rest[-14:]
    az, odd = position()

    @pl.when((az == 0) if late else (az > 0))
    def _():
        small = start_all(
            (lines_hbm, lines_ref, small_sems.at[0]),
            (cols_hbm, cols_ref, small_sems.at[1]),
            (couples_hbm, couples_ref, small_sems.at[2]),
            (curve_hbm, curve_ref, small_sems.at[3]),
        )
        planes = start_all(
            *(
                (x_hbm.at[p // IMAGES, p % IMAGES, 0], x.at[p], sems.at[p])
                for p in range(PLANES)
            )
        )
        wait_all(small)
        offset = az * BLOCK_HEIGHT - start_ref[0]
        last = BLOCK_HEIGHT - MARGIN

        def take(row, out_ref, wait):
            base = window_base(offset + row)

            def window(p):
                if wait:
                    planes[p].wait()
                return x.at[p, pl.ds(base, WINDOW)]

            take_lines(offset + row, base, window, lines_ref, cols_ref, curve_ref, out_ref)

        take(jnp.where(odd, last, 0), b_out, True)
        take(jnp.where(odd, 0, last), a_out, False)
        take(MARGIN, middle, False)
        sums = box_sums(4, BOXES - 2 * (MARGIN // LOOK_ROWS), (middle,), couples_ref, merged)
        for u in range(3 * PAIRS):
            sums_out[u] = pltpu.roll(sums[u], MARGIN // LOOK_ROWS, 0)


def add_edge(low, sums, sums_ref):
    edge = MARGIN // LOOK_ROWS
    sublane = iota((BOXES, LOOKS), 0)
    first = jnp.where(low, 0, BOXES - edge)
    mine = (sublane >= first) & (sublane < first + edge)
    return [
        jnp.where(
            mine, jnp.where(low, sums[u], pltpu.roll(sums[u], BOXES - edge, 0)), sums_ref[u]
        )
        for u in range(3 * PAIRS)
    ]


def far_kernel(
    couples_vmem, b_ref, own_ref, sums_ref, out_ref, couples_ref, sem, *merged
):
    _, odd = position()
    copies = start_all((couples_vmem, couples_ref, sem))
    sums = box_sums(
        2,
        MARGIN // LOOK_ROWS,
        (b_ref, own_ref),
        couples_ref,
        merged,
        ready=lambda: wait_all(copies),
    )
    for u, value in enumerate(add_edge(jnp.logical_not(odd), sums, sums_ref)):
        out_ref[u] = value


def near_kernel(
    couples_vmem, a_ref, own_ref, sums_ref, ifg_ref, coh_ref, power, couples_ref, sem, *merged
):
    _, odd = position()
    copies = start_all((couples_vmem, couples_ref, sem))
    sums = box_sums(
        2,
        MARGIN // LOOK_ROWS,
        (a_ref, own_ref),
        couples_ref,
        merged,
        ready=lambda: wait_all(copies),
    )
    sums = add_edge(odd, sums, sums_ref)
    for a in range(IMAGES):
        power[a] = sums[2 * PAIRS + a]
    for p in range(PAIRS):
        re, im = sums[p], sums[PAIRS + p]
        ifg_ref[0, p] = re / float(LOOK_ROWS * LOOK_COLS)
        ifg_ref[1, p] = im / float(LOOK_ROWS * LOOK_COLS)
        both = power[couples_ref[p, 0]] * power[couples_ref[p, 1]]
        coh_ref[p] = (re * re + im * im) / jnp.maximum(both, 1.0)


def swaps(n, first):
    pairs = [(k, k + 1) for k in range(first, n - 1, 2)]
    return pairs + [(j, i) for i, j in pairs]


def limit(mebibytes):
    return pltpu.CompilerParams(vmem_limit_bytes=mebibytes * 2**20)


def in_hbm(array):
    return pltpu.with_memory_space_constraint(array, pltpu.HBM)


def per_device(
    sweep_stack,
    blend_curve,
    sweep_start_index,
    usable_azimuth_extent,
    usable_column_extent,
    image_couples,
):
    n = lax.axis_size("az")
    sent = jax.ShapeDtypeStruct((PLANES, SENT, SLANT_WIDTH), BF16)
    sums_shape = jax.ShapeDtypeStruct((3 * PAIRS, BOXES, LOOKS), F32)
    dma = pltpu.SemaphoreType.DMA
    lines_smem = pltpu.SMEM((1, 2), jnp.int32)
    couples_smem = pltpu.SMEM((PAIRS, 2), jnp.int32)
    curve_vmem = pltpu.VMEM((1, SWEEP_HEIGHT), BF16)
    merged = [
        pltpu.VMEM((2, IMAGES, BLOCK_HEIGHT, TILE), F32) for _ in range(SLANT_WIDTH // 2 // TILE)
    ]
    lines, columns, couples, curve, stack = (
        in_hbm(array)
        for array in (
            usable_azimuth_extent,
            usable_column_extent,
            image_couples,
            blend_curve,
            sweep_stack,
        )
    )
    to_a, to_b = pl.pallas_call(
        pack_kernel,
        out_shape=(sent, sent),
        in_specs=[SMEM] + [HBM] * 4,
        out_specs=(VMEM, VMEM),
        scratch_shapes=[
            pltpu.VMEM((2, PLANES, WINDOW, SLANT_WIDTH), BF16),
            lines_smem,
            lines_smem,
            curve_vmem,
            dma((2, PLANES)),
            dma((3,)),
        ],
        compiler_params=limit(16),
        name="pack",
    )(sweep_start_index, lines, columns, curve, stack)
    from_b = lax.ppermute(to_b, "az", swaps(n, 1))
    from_a = lax.ppermute(to_a, "az", swaps(n, 0))

    def own(late, *before):
        return pl.pallas_call(
            functools.partial(own_kernel, late),
            out_shape=(sent, sent, sums_shape),
            in_specs=[SMEM] + [HBM] * 5 + [VMEM] * len(before),
            out_specs=(VMEM, VMEM, VMEM),
            scratch_shapes=[
                pltpu.VMEM((PLANES, SWEEP_HEIGHT, SLANT_WIDTH), BF16),
                pltpu.VMEM((PLANES, SENT, SLANT_WIDTH), BF16),
                lines_smem,
                lines_smem,
                couples_smem,
                curve_vmem,
                *merged[:3],
                dma((4,)),
                dma((PLANES,)),
            ],
            input_output_aliases={6: 0, 7: 1, 8: 2} if before else {},
            compiler_params=limit(24),
            name="late" if late else "early",
        )(sweep_start_index, lines, columns, couples, curve, stack, *before)

    own_a, own_b, sums = own(False)
    own_a, own_b, sums = own(True, own_a, own_b, sums)
    sums = pl.pallas_call(
        far_kernel,
        out_shape=sums_shape,
        in_specs=[VMEM, VMEM, VMEM, VMEM],
        out_specs=VMEM,
        scratch_shapes=[couples_smem, dma, *merged],
        compiler_params=limit(16),
        name="far",
    )(image_couples, from_b, own_b, sums)
    return pl.pallas_call(
        near_kernel,
        out_shape=(
            jax.ShapeDtypeStruct((2, PAIRS, BOXES, LOOKS), F32),
            jax.ShapeDtypeStruct((PAIRS, BOXES, LOOKS), F32),
        ),
        in_specs=[VMEM, VMEM, VMEM, VMEM],
        out_specs=(VMEM, VMEM),
        scratch_shapes=[pltpu.VMEM((IMAGES, BOXES, LOOKS), F32), couples_smem, dma, *merged],
        compiler_params=limit(16),
        name="near",
    )(image_couples, from_a, own_a, sums)


def solution(mesh):
    return jax.shard_map(
        per_device,
        mesh=mesh,
        in_specs=(
            P(None, None, ("groups", "az"), None, None),
            P(("groups", "az"), None),
            P(("groups", "az")),
            P(("groups", "az"), None),
            P(("groups", "az"), None),
            P("groups", None),
        ),
        out_specs=(P(None, "groups", "az", None), P("groups", "az", None)),
        check_vma=False,
    )
```

```python
import functools

import jax
import jax.numpy as jnp
from jax import lax
from jax.experimental import pallas as pl
from jax.experimental.pallas import tpu as pltpu
from jax.sharding import PartitionSpec as P

BLOCK_HEIGHT = 40
SLANT_WIDTH = 2560
LOOK_ROWS = 5
LOOK_COLS = 20
MARGIN = 15
SWEEP_HEIGHT = 80
IMAGES = 4
PLANES = 2 * IMAGES
PAIRS = 4
SENT = 16
WINDOW = 32
LOOKS = SLANT_WIDTH // LOOK_COLS
BOXES = BLOCK_HEIGHT // LOOK_ROWS
TILE = 256
TILES = SLANT_WIDTH // TILE
F32 = jnp.float32
BF16 = jnp.bfloat16

HBM = pl.BlockSpec(memory_space=pltpu.HBM)
VMEM = pl.BlockSpec(memory_space=pltpu.VMEM)
SMEM = pl.BlockSpec(memory_space=pltpu.SMEM)


def iota(shape, dim):
    return lax.broadcasted_iota(jnp.int32, shape, dim)


def as_bf16(mask):
    return mask.astype(F32).astype(BF16)


def position():
    az = lax.axis_index("az")
    return az, lax.rem(az, 2) == 1


def columns_inside(cols_ref, first, count):
    col = iota((1, count), 1) + first
    return as_bf16((col >= cols_ref[0, 0]) & (col < cols_ref[0, 1]))


def window_base(first):
    base = lax.shift_left(lax.shift_right_arithmetic(first, 4), 4)
    return pl.multiple_of(jnp.clip(base, 0, SWEEP_HEIGHT - WINDOW), 16)


def take_lines(first, base, window, lines_ref, cols_ref, curve_ref, out_ref):
    line = iota((SWEEP_HEIGHT, 128), 0)
    place = iota((SWEEP_HEIGHT, 128), 1)
    chosen = (
        (line == first + place)
        & (place < MARGIN)
        & (line >= lines_ref[0, 0])
        & (line < lines_ref[0, 1])
    )
    curve = jnp.broadcast_to(curve_ref[...], (SENT, SWEEP_HEIGHT))
    weights = jnp.dot(curve, as_bf16(chosen), preferred_element_type=F32).astype(BF16)
    row = iota((SENT, WINDOW), 0)
    source = iota((SENT, WINDOW), 1) + base
    pick = as_bf16((source == first + row) & (row < MARGIN))
    inside = columns_inside(cols_ref, 0, SLANT_WIDTH)
    for p in range(PLANES):
        lines = window(p)
        for t in range(TILES):
            cols = slice(t * TILE, (t + 1) * TILE)
            block = jnp.dot(pick, lines[:, cols], preferred_element_type=F32)
            out_ref[p, :, cols] = block.astype(BF16) * inside[:, cols]
    last = iota((SENT, 128), 0) == MARGIN
    out_ref[0, :, :128] = jnp.where(last, weights, out_ref[0, :, :128])


def start_all(*pairs):
    copies = [pltpu.make_async_copy(source, target, sem) for source, target, sem in pairs]
    for copy in copies:
        copy.start()
    return copies


def wait_all(copies):
    for copy in copies:
        copy.wait()


def pack_kernel(
    start_ref,
    lines_hbm,
    cols_hbm,
    curve_hbm,
    x_hbm,
    a_ref,
    b_ref,
    windows,
    lines_ref,
    cols_ref,
    curve_ref,
    sems,
    small_sems,
):
    az, odd = position()
    offset = az * BLOCK_HEIGHT - start_ref[0]
    down = offset - MARGIN
    up = offset + BLOCK_HEIGHT
    firsts = (jnp.where(odd, down, up), jnp.where(odd, up, down))
    bases = [window_base(first) for first in firsts]

    def fetch(side):
        rows = pl.ds(bases[side], WINDOW)
        return start_all(
            *(
                (
                    x_hbm.at[p // IMAGES, p % IMAGES, 0, rows, :],
                    windows.at[side, p],
                    sems.at[side, p],
                )
                for p in range(PLANES)
            )
        )

    near = fetch(0)
    small = start_all(
        (lines_hbm, lines_ref, small_sems.at[0]),
        (cols_hbm, cols_ref, small_sems.at[1]),
        (curve_hbm, curve_ref, small_sems.at[2]),
    )
    wait_all(small)

    def take(side, copies, out_ref):
        wait_all(copies)
        take_lines(
            firsts[side],
            bases[side],
            lambda p: windows.at[side, p],
            lines_ref,
            cols_ref,
            curve_ref,
            out_ref,
        )

    take(0, near, a_ref)

    @pl.when((az > 0) & (az < lax.axis_size("az") - 1))
    def _():
        take(1, fetch(1), b_ref)


def weights_of(ref):
    return ref[0, MARGIN:SENT, :SENT].astype(F32)


def box_sums(parts, boxes, sources, cells_ref, couples_ref, merged_refs, ready=None):
    stride = BOXES // parts
    width = SLANT_WIDTH // parts
    slot = iota((BLOCK_HEIGHT, SENT), 0)
    place = iota((BLOCK_HEIGHT, SENT), 1)
    box = slot & (stride - 1)
    part = (slot & 7) // stride
    match = (place == box * LOOK_ROWS + (slot >> 3)) & (box < boxes)
    chosen = [jnp.where(match, weights_of(ref), 0.0) for ref in sources]
    total = jnp.sum(sum(chosen), axis=1, keepdims=True)
    scale = jnp.where(total > 0.0, 1.0 / total, 0.0)
    scale = jnp.broadcast_to(scale, (BLOCK_HEIGHT, TILE))
    select = jnp.concatenate(
        [jnp.where(part == q, w, 0.0) for q in range(parts) for w in chosen], axis=1
    ).astype(BF16)
    tiles = [(at, min(TILE, width - at)) for at in range(0, width, TILE)]

    def merge(t):
        (at, size), merged = tiles[t], merged_refs[t]
        for p in range(PLANES):
            values = jnp.concatenate(
                [
                    ref[p, :, q * width + at : q * width + at + size]
                    for q in range(parts)
                    for ref in sources
                ],
                axis=0,
            )
            merged[p // IMAGES, p % IMAGES, :, :size] = (
                jnp.dot(select, values, preferred_element_type=F32) * scale[:, :size]
            )

    def look(t, couples):
        (at, size), merged = tiles[t], merged_refs[t]

        def rows(v):
            return jnp.sum(v.reshape(LOOK_ROWS, BOXES, size), axis=0)

        def plane(c, image):
            return merged[c, image, :, :size]

        real, imag, powers = [], [], []
        for i, j in couples:
            ri, ii, rj, ij = plane(0, i), plane(1, i), plane(0, j), plane(1, j)
            real.append(rows(ri * rj + ii * ij))
            imag.append(rows(ii * rj - ri * ij))
        for a in range(IMAGES):
            re, im = plane(0, a), plane(1, a)
            powers.append(rows(re * re + im * im))
        sums = jnp.concatenate(real + imag + powers, axis=0)
        high = sums.astype(BF16)
        low = (sums - high.astype(F32)).astype(BF16)
        cells = cells_ref[at : at + size, :]
        return jnp.dot(high, cells, preferred_element_type=F32) + jnp.dot(
            low, cells, preferred_element_type=F32
        )

    merge(0)
    merge(1)
    if ready is not None:
        ready()
    couples = [(couples_ref[0, p], couples_ref[1, p]) for p in range(PAIRS)]
    acc = None
    for t in range(len(tiles)):
        if t + 2 < len(tiles):
            merge(t + 2)
        got = look(t, couples)
        acc = got if acc is None else acc + got
    lane = iota((BOXES, LOOKS), 1)
    step = LOOKS // parts
    out = []
    for u in range(3 * PAIRS):
        got = acc[u * BOXES : (u + 1) * BOXES, :]
        whole = got
        for q in range(1, parts):
            moved = pltpu.roll(pltpu.roll(got, q * step, 1), BOXES - q * stride, 0)
            whole = jnp.where(lane >= q * step, moved, whole)
        out.append(whole)
    return out


def own_kernel(
    late,
    start_ref,
    lines_hbm,
    cols_hbm,
    couples_hbm,
    curve_hbm,
    x_hbm,
    *rest,
):
    (
        a_out,
        b_out,
        sums_out,
        cells_out,
        x,
        middle,
        lines_ref,
        cols_ref,
        couples_ref,
        curve_ref,
        *merged,
        small_sems,
        sems,
    ) = rest[-15:]
    az, odd = position()

    @pl.when((az == 0) if late else (az > 0))
    def _():
        small = start_all(
            (lines_hbm, lines_ref, small_sems.at[0]),
            (cols_hbm, cols_ref, small_sems.at[1]),
            (couples_hbm, couples_ref, small_sems.at[2]),
            (curve_hbm, curve_ref, small_sems.at[3]),
        )
        planes = start_all(
            *(
                (x_hbm.at[p // IMAGES, p % IMAGES, 0], x.at[p], sems.at[p])
                for p in range(PLANES)
            )
        )
        wait_all(small + planes)
        offset = az * BLOCK_HEIGHT - start_ref[0]
        last = BLOCK_HEIGHT - MARGIN

        def take(row, out_ref):
            base = window_base(offset + row)

            take_lines(
                offset + row,
                base,
                lambda p: x.at[p, pl.ds(base, WINDOW)],
                lines_ref,
                cols_ref,
                curve_ref,
                out_ref,
            )

        take(jnp.where(odd, last, 0), b_out)
        take(jnp.where(odd, 0, last), a_out)
        take(MARGIN, middle)
        for at in range(0, SLANT_WIDTH // 2, TILE):
            where = iota((TILE, LOOKS), 0) + at
            look = iota((TILE, LOOKS), 1) * LOOK_COLS
            cells_out[at : at + TILE, :] = as_bf16((where >= look) & (where < look + LOOK_COLS))
        boxes = BOXES - 2 * (MARGIN // LOOK_ROWS)
        sums = box_sums(4, boxes, (middle,), cells_out, couples_ref, merged)
        for u in range(3 * PAIRS):
            sums_out[u] = pltpu.roll(sums[u], MARGIN // LOOK_ROWS, 0)


def add_edge(low, sums, sums_ref):
    edge = MARGIN // LOOK_ROWS
    sublane = iota((BOXES, LOOKS), 0)
    first = jnp.where(low, 0, BOXES - edge)
    mine = (sublane >= first) & (sublane < first + edge)
    return [
        jnp.where(
            mine, jnp.where(low, sums[u], pltpu.roll(sums[u], BOXES - edge, 0)), sums_ref[u]
        )
        for u in range(3 * PAIRS)
    ]


def far_kernel(
    couples_vmem, b_ref, own_ref, sums_ref, cells_ref, out_ref, couples_ref, sem, *merged
):
    _, odd = position()
    copies = start_all((couples_vmem, couples_ref, sem))
    sums = box_sums(
        2,
        MARGIN // LOOK_ROWS,
        (b_ref, own_ref),
        cells_ref,
        couples_ref,
        merged,
        ready=lambda: wait_all(copies),
    )
    for u, value in enumerate(add_edge(jnp.logical_not(odd), sums, sums_ref)):
        out_ref[u] = value


def near_kernel(
    couples_vmem,
    a_ref,
    own_ref,
    sums_ref,
    cells_ref,
    ifg_ref,
    coh_ref,
    power,
    couples_ref,
    sem,
    *merged,
):
    _, odd = position()
    copies = start_all((couples_vmem, couples_ref, sem))
    sums = box_sums(
        2,
        MARGIN // LOOK_ROWS,
        (a_ref, own_ref),
        cells_ref,
        couples_ref,
        merged,
        ready=lambda: wait_all(copies),
    )
    sums = add_edge(odd, sums, sums_ref)
    for a in range(IMAGES):
        power[a] = sums[2 * PAIRS + a]
    for p in range(PAIRS):
        re, im = sums[p], sums[PAIRS + p]
        ifg_ref[0, p] = re / float(LOOK_ROWS * LOOK_COLS)
        ifg_ref[1, p] = im / float(LOOK_ROWS * LOOK_COLS)
        both = power[couples_ref[0, p]] * power[couples_ref[1, p]]
        coh_ref[p] = (re * re + im * im) / jnp.maximum(both, 1.0)


def swaps(n, first):
    pairs = [(k, k + 1) for k in range(first, n - 1, 2)]
    return pairs + [(j, i) for i, j in pairs]


def limit(mebibytes):
    return pltpu.CompilerParams(vmem_limit_bytes=mebibytes * 2**20)


def in_hbm(array):
    return pltpu.with_memory_space_constraint(array, pltpu.HBM)


def per_device(
    sweep_stack,
    blend_curve,
    sweep_start_index,
    usable_azimuth_extent,
    usable_column_extent,
    image_couples,
):
    n = lax.axis_size("az")
    sent = jax.ShapeDtypeStruct((PLANES, SENT, SLANT_WIDTH), BF16)
    sums_shape = jax.ShapeDtypeStruct((3 * PAIRS, BOXES, LOOKS), F32)
    cells_shape = jax.ShapeDtypeStruct((SLANT_WIDTH // 2, LOOKS), BF16)
    dma = pltpu.SemaphoreType.DMA
    lines_smem = pltpu.SMEM((1, 2), jnp.int32)
    couples_smem = pltpu.SMEM((2, PAIRS), jnp.int32)
    curve_vmem = pltpu.VMEM((1, SWEEP_HEIGHT), BF16)
    merged = [
        pltpu.VMEM((2, IMAGES, BLOCK_HEIGHT, TILE), F32) for _ in range(SLANT_WIDTH // 2 // TILE)
    ]
    couples = image_couples.T
    lines, columns, couples_hbm, curve, stack = (
        in_hbm(array)
        for array in (
            usable_azimuth_extent,
            usable_column_extent,
            couples,
            blend_curve,
            sweep_stack,
        )
    )
    to_a, to_b = pl.pallas_call(
        pack_kernel,
        out_shape=(sent, sent),
        in_specs=[SMEM] + [HBM] * 4,
        out_specs=(VMEM, VMEM),
        scratch_shapes=[
            pltpu.VMEM((2, PLANES, WINDOW, SLANT_WIDTH), BF16),
            lines_smem,
            lines_smem,
            curve_vmem,
            dma((2, PLANES)),
            dma((3,)),
        ],
        compiler_params=limit(16),
        name="pack",
    )(sweep_start_index, lines, columns, curve, stack)
    from_b = lax.ppermute(to_b, "az", swaps(n, 1))
    from_a = lax.ppermute(to_a, "az", swaps(n, 0))

    def own(late, *before):
        return pl.pallas_call(
            functools.partial(own_kernel, late),
            out_shape=(sent, sent, sums_shape, cells_shape),
            in_specs=[SMEM] + [HBM] * 5 + [VMEM] * len(before),
            out_specs=(VMEM,) * 4,
            scratch_shapes=[
                pltpu.VMEM((PLANES, SWEEP_HEIGHT, SLANT_WIDTH), BF16),
                pltpu.VMEM((PLANES, SENT, SLANT_WIDTH), BF16),
                lines_smem,
                lines_smem,
                couples_smem,
                curve_vmem,
                *merged[:3],
                dma((4,)),
                dma((PLANES,)),
            ],
            input_output_aliases={6 + k: k for k in range(len(before))},
            compiler_params=limit(24),
            name="late" if late else "early",
        )(sweep_start_index, lines, columns, couples_hbm, curve, stack, *before)

    mine = own(False)
    own_a, own_b, sums, cells = own(True, *mine)
    sums = pl.pallas_call(
        far_kernel,
        out_shape=sums_shape,
        in_specs=[VMEM] * 5,
        out_specs=VMEM,
        scratch_shapes=[couples_smem, dma, *merged],
        compiler_params=limit(16),
        name="far",
    )(couples, from_b, own_b, sums, cells)
    return pl.pallas_call(
        near_kernel,
        out_shape=(
            jax.ShapeDtypeStruct((2, PAIRS, BOXES, LOOKS), F32),
            jax.ShapeDtypeStruct((PAIRS, BOXES, LOOKS), F32),
        ),
        in_specs=[VMEM] * 5,
        out_specs=(VMEM, VMEM),
        scratch_shapes=[pltpu.VMEM((IMAGES, BOXES, LOOKS), F32), couples_smem, dma, *merged],
        compiler_params=limit(16),
        name="near",
    )(couples, from_a, own_a, sums, cells)


def solution(mesh):
    return jax.shard_map(
        per_device,
        mesh=mesh,
        in_specs=(
            P(None, None, ("groups", "az"), None, None),
            P(("groups", "az"), None),
            P(("groups", "az")),
            P(("groups", "az"), None),
            P(("groups", "az"), None),
            P("groups", None),
        ),
        out_specs=(P(None, "groups", "az", None), P("groups", "az", None)),
        check_vma=False,
    )
```
